16 devices in a mesh: dp: 2 (over y, z), tp: 8 (over x, core).
Axes of the slice: x: 4, y: 2, z: 1, core: 2. Of those that a mesh axis runs over, the one named last changes fastest.
The devices are a block of a 4x4x8 slice.
Arguments:
- x: bfloat16 [4096, 8192], P('dp'), parts along dimension 0
- w_gate: bfloat16 [8192, 32768], P(None, 'tp')
- w_up: bfloat16 [8192, 32768], P(None, 'tp')
- w_down: bfloat16 [32768, 8192], P('tp')
Outputs:
- output: bfloat16 [4096, 8192], P('dp'), parts along dimension 0
There are 2 independent parts. The reference program is written for one: setup_inputs(seed, part) draws one part's arguments, and reference() takes and returns one part's arrays. A program takes and returns all parts, laid end to end along the dimension named above; an argument that names none is the same for every part.
All inputs are finite; a program needn't handle non-finite values.
Results may differ from the reference program's by a relative error of at most 0.016.
Values are sent between devices in bfloat16 or wider.
A program may use at most 768 MiB of HBM per device.

```python
import jax
import jax.numpy as jnp

ROWS = 2048
D = 8192
FF = 32768


def setup_inputs(seed: int = 0, part: int = 0) -> dict:
    kx, kg, ku, kd = jax.random.split(jax.random.key(seed), 4)
    drawn = {
        "x": jax.random.normal(jax.random.fold_in(kx, part), (ROWS, D), jnp.float32),
        "w_gate": jax.random.normal(kg, (D, FF), jnp.float32) * D**-0.5,
        "w_up": jax.random.normal(ku, (D, FF), jnp.float32) * D**-0.5,
        "w_down": jax.random.normal(kd, (FF, D), jnp.float32) * FF**-0.5,
    }
    return {k: v.astype(jnp.bfloat16) for k, v in drawn.items()}


def reference(x, w_gate, w_up, w_down):
    gate = jnp.dot(x, w_gate, preferred_element_type=jnp.float32)
    up = jnp.dot(x, w_up, preferred_element_type=jnp.float32)
    hidden = (jax.nn.silu(gate) * up).astype(jnp.bfloat16)
    return jnp.dot(hidden, w_down, preferred_element_type=jnp.float32).astype(jnp.bfloat16)
```

```python
import functools

import jax
import jax.numpy as jnp
from jax import lax
from jax.experimental import pallas as pl
from jax.experimental.pallas import tpu as pltpu
from jax.sharding import PartitionSpec as P

MESH = pl.DeviceIdType.MESH
BF16, F32 = jnp.bfloat16, jnp.float32

CHUNK = 512
GU = 256
DN = 512

OTHER, OWN = 0, 1
ORDER = (
    (OTHER, 2, 0), (OTHER, 2, 1), (OTHER, 3, 0), (OWN, 2, 0), (OWN, 2, 1), (OTHER, 3, 1), (OTHER, 1, 0), (OTHER, 1, 1),
    (OWN, 3, 1), (OWN, 1, 0), (OTHER, 0, 0), (OTHER, 0, 1), (OWN, 3, 0), (OWN, 1, 1), (OWN, 0, 0), (OWN, 0, 1),
)
TILES = len(ORDER)
STAGED = TILES - 2
RING = {3: (-1, 0), 4: (1, 1), 8: (-1, 3), 9: (1, 4), 12: (-1, 2), 13: (1, 5)}
FIRST = 2


def pick(t, values):
    out = jnp.int32(values[0])
    for k, v in enumerate(values[1:], 1):
        if v != values[0]:
            out = jnp.where(t == k, jnp.int32(v), out)
    return out


def kernel(chips, chunks, x_ref, wg_ref, wu_ref, wd_ref, y_ref, x_v, hid, wg_v, wu_v, wd_v, g0, u0, g1, u1, a0, a1,
           other, hop1, hop2, stage, fin, x_sem, wg_sem, wu_sem, wd_sem, send_sem, other_sem, ring_sem, gsend_sem,
           gather_sem, credit):
    dp, tp = lax.axis_index("dp"), lax.axis_index("tp")
    chip, core = tp // 2, tp % 2
    nxt, prv = (chip + 1) % chips, (chip + chips - 1) % chips
    far = (chip + 2) % chips
    dev_next, dev_prev, dev_other = (dp, nxt * 2 + core), (dp, prv * 2 + core), (dp, chip * 2 + 1 - core)
    n_gu = wg_ref.shape[1] // GU
    last = chunks - 1

    barrier = pltpu.get_barrier_semaphore()
    for dev in (dev_next, dev_prev, dev_other):
        pl.semaphore_signal(barrier, inc=1, device_id=dev, device_id_type=MESH)
    pl.semaphore_wait(barrier, 3)

    def rows(chunk):
        return pl.ds(pl.multiple_of(chunk * CHUNK, CHUNK), CHUNK)

    def x_copy(chunk):
        return pltpu.make_async_copy(x_ref.at[rows(chunk), :], x_v, x_sem)

    def gu_copies(j, slot):
        cols = pl.ds(pl.multiple_of(j * GU, GU), GU)
        return (pltpu.make_async_copy(wg_ref.at[:, cols], wg_v.at[slot], wg_sem.at[slot]),
                pltpu.make_async_copy(wu_ref.at[:, cols], wu_v.at[slot], wu_sem.at[slot]))

    def block(half, owner, piece):
        return (half * chips + owner) * 2 + piece

    def wd_copy(t, slot):
        half = jnp.where(pick(t, [o[0] for o in ORDER]) == OWN, core, 1 - core)
        owner = (chip + pick(t, [o[1] for o in ORDER])) % chips
        tile = block(half, owner, pick(t, [o[2] for o in ORDER]))
        cols = pl.ds(pl.multiple_of(tile * DN, DN), DN)
        return pltpu.make_async_copy(wd_ref.at[:, cols], wd_v.at[slot], wd_sem.at[slot])

    def remote(src, dst, send, recv, dev):
        return pltpu.make_async_remote_copy(src_ref=src, dst_ref=dst, send_sem=send, recv_sem=recv, device_id=dev,
                                            device_id_type=MESH)

    def other_copy(chunk, t, slot):
        return remote(stage.at[t], other.at[slot], send_sem.at[t], other_sem.at[chunk, slot], dev_other)

    def ring_copy(chunk, t):
        direction, slot = RING[t]
        dst = hop1.at[slot] if slot < FIRST else hop2.at[slot - FIRST]
        return remote(stage.at[t], dst, send_sem.at[t], ring_sem.at[chunk, slot], dev_next if direction > 0 else dev_prev)

    def out(chunk, owner, half=core, piece=None):
        if piece is None:
            return y_ref.at[rows(chunk), pl.ds(pl.multiple_of(block(half, owner, 0) * DN, 2 * DN), 2 * DN)]
        return y_ref.at[rows(chunk), pl.ds(pl.multiple_of(block(half, owner, piece) * DN, DN), DN)]

    def gathers(chunk):
        def put(src, dst, k, slot, dev):
            return remote(src, dst, gsend_sem.at[k], gather_sem.at[chunk, slot], dev)

        mine = out(chunk, chip)
        first = (put(fin, mine, 1, 4, dev_other), put(fin, mine, 2, 0, dev_next), put(fin, mine, 3, 1, dev_prev))
        a, b = out(chunk, prv, piece=0), out(chunk, nxt, piece=1)
        p, n = out(chunk, prv), out(chunk, nxt)
        second = (put(a, a, 4, 2, dev_next), put(b, b, 5, 3, dev_prev), put(p, p, 6, 5, dev_other),
                  put(n, n, 7, 6, dev_other))
        fa, fb = out(chunk, far, piece=0), out(chunk, far, piece=1)
        third = (put(fa, fa, 8, 7, dev_other), put(fb, fb, 9, 8, dev_other))
        return pltpu.make_async_copy(fin, mine, gsend_sem.at[0]), first, second, third

    def gather_wait(chunk, slot, dst):
        remote(dst, dst, gsend_sem.at[0], gather_sem.at[chunk, slot], dev_other).wait_recv()

    def sent(chunk):
        local, first, second, third = gathers(chunk)
        local.wait()
        for copy in first + second + third:
            copy.wait_send()

    def finish(chunk):
        for slot in range(2):
            remote(stage.at[0], other.at[slot], send_sem.at[0], other_sem.at[chunk, slot], dev_other).wait_recv()
        for k in range(4):
            remote(stage.at[0], hop2.at[k], send_sem.at[0], ring_sem.at[chunk, FIRST + k], dev_next).wait_recv()

        @pl.when(chunk > 0)
        def _():
            sent(chunk - 1)

        step = 64

        def strip(i, _):
            r = pl.ds(pl.multiple_of(i * step, step), step)
            for piece, acc in ((0, a0), (1, a1)):
                total = acc[r, :] + other[piece, r, :].astype(F32)
                total += hop2[piece, r, :].astype(F32)
                total += hop2[2 + piece, r, :].astype(F32)
                fin[r, piece * DN:(piece + 1) * DN] = total.astype(BF16)
            return 0

        lax.fori_loop(0, CHUNK // step, strip, 0)
        local, first, _, _ = gathers(chunk)
        for copy in (first[1], first[2], first[0], local):
            copy.start()

        @pl.when(chunk < last)
        def _():
            for k, dev in enumerate((dev_prev, dev_next, dev_other)):
                pl.semaphore_signal(credit.at[k], inc=1, device_id=dev, device_id_type=MESH)

    def forward1(chunk):
        gather_wait(chunk, 0, out(chunk, prv))
        gather_wait(chunk, 1, out(chunk, nxt))
        for copy in gathers(chunk)[2]:
            copy.start()

    def forward2(chunk):
        gather_wait(chunk, 2, out(chunk, far, piece=0))
        gather_wait(chunk, 3, out(chunk, far, piece=1))
        for copy in gathers(chunk)[3]:
            copy.start()

    def activate(g, u, j):
        cols = pl.ds(pl.multiple_of(j * GU, GU), GU)
        gate = g[...]
        hid[:, cols] = (gate * jax.nn.sigmoid(gate) * u[...]).astype(BF16)

    def gu_tile(slot, g, u, g_old, u_old, j_old):
        g[...] = jnp.dot(x_v[...], wg_v[slot], preferred_element_type=F32)
        u[...] = jnp.dot(x_v[...], wu_v[slot], preferred_element_type=F32)
        activate(g_old, u_old, j_old)

    def dn_tile(chunk, t, slot, acc, acc_old):
        old = t - 1
        staged = (old >= 0) & (old < STAGED)
        is_own = [o[0] == OWN for o in ORDER[:STAGED]]
        own = staged & (pick(old, [int(f) for f in is_own]) == 1)
        slots = [o[1] * 2 + o[2] for o in ORDER]
        arrived = pick(old, slots)

        @pl.when(staged & (chunk > 0))
        def _():
            remote(stage.at[old], other.at[0], send_sem.at[old], other_sem.at[chunk, 0], dev_other).wait_send()

        @pl.when(own)
        def _():
            remote(stage.at[0], other.at[arrived], send_sem.at[0], other_sem.at[chunk, arrived], dev_other).wait_recv()

        for k, at in ((0, 12), (1, 13)):
            @pl.when(old == at)
            def _(k=k):
                remote(stage.at[0], hop1.at[k], send_sem.at[0], ring_sem.at[chunk, k], dev_next).wait_recv()

        from_other = jnp.where(own, arrived, len(ORDER) // 2)
        from_ring = jnp.where(old == 12, 0, jnp.where(old == 13, 1, 2))
        to = jnp.where(staged, old, STAGED)
        acc[...] = jnp.dot(hid[...], wd_v[slot], preferred_element_type=F32)
        total = acc_old[...] + other[from_other].astype(F32) + hop1[from_ring].astype(F32)
        stage[to] = total.astype(BF16)

        @pl.when(staged & jnp.logical_not(own))
        def _():
            other_copy(chunk, old, arrived).start()

        for at in RING:
            @pl.when(old == at)
            def _(at=at):
                ring_copy(chunk, at).start()

    x_copy(0).start()
    for copy in gu_copies(0, 0):
        copy.start()
    other[len(ORDER) // 2] = jnp.zeros(other.shape[1:], BF16)
    hop1[FIRST] = jnp.zeros(hop1.shape[1:], BF16)

    def one_chunk(chunk, _):
        x_copy(chunk).wait()

        def gu_pair(i, _):
            j = i * 2
            for copy in gu_copies(j, 0):
                copy.wait()
            for copy in gu_copies(j + 1, 1):
                copy.start()
            gu_tile(0, g0, u0, g1, u1, (j + n_gu - 1) % n_gu)
            for copy in gu_copies(j + 1, 1):
                copy.wait()

            @pl.when(j + 2 < n_gu)
            def _():
                for copy in gu_copies(j + 2, 0):
                    copy.start()

            @pl.when(j + 2 >= n_gu)
            def _():
                wd_copy(jnp.int32(0), 0).start()

            for at, act in ((1, finish), (4, forward1), (6, forward2)):
                @pl.when((i == at) & (chunk > 0))
                def _(act=act):
                    act(chunk - 1)

            gu_tile(1, g1, u1, g0, u0, j)
            return 0

        lax.fori_loop(0, n_gu // 2, gu_pair, 0)
        activate(g1, u1, n_gu - 1)

        @pl.when(chunk > 0)
        def _():
            for k in range(3):
                pl.semaphore_wait(credit.at[k], 1)

        @pl.when(chunk < last)
        def _():
            x_copy(chunk + 1).start()

        def dn_pair(i, _):
            t = i * 2
            wd_copy(t, 0).wait()
            wd_copy(t + 1, 1).start()
            dn_tile(chunk, t, 0, a0, a1)
            wd_copy(t + 1, 1).wait()

            @pl.when(t + 2 < TILES)
            def _():
                wd_copy(t + 2, 0).start()

            @pl.when((t + 2 >= TILES) & (chunk < last))
            def _():
                for copy in gu_copies(0, 0):
                    copy.start()

            dn_tile(chunk, t + 1, 1, a1, a0)
            return 0

        lax.fori_loop(0, TILES // 2, dn_pair, 0)
        return 0

    lax.fori_loop(0, chunks, one_chunk, 0)
    finish(last)
    forward1(last)
    forward2(last)
    sent(last)
    for t in range(STAGED):
        remote(stage.at[t], other.at[0], send_sem.at[t], other_sem.at[last, 0], dev_other).wait_send()
    for chunk in range(chunks):
        half = 1 - core
        for slot, dst in ((4, out(chunk, chip, half)), (5, out(chunk, prv, half)), (6, out(chunk, nxt, half)),
                          (7, out(chunk, far, half, 0)), (8, out(chunk, far, half, 1))):
            gather_wait(chunk, slot, dst)


def solution(mesh):
    chips = mesh.shape["tp"] // 2

    def step(x, w_gate, w_up, w_down):
        n, d = x.shape
        ff = w_gate.shape[1]
        chunks = n // CHUNK
        dma = pltpu.SemaphoreType.DMA
        hbm = pl.BlockSpec(memory_space=pl.ANY)
        return pl.pallas_call(
            functools.partial(kernel, chips, chunks),
            out_shape=jax.ShapeDtypeStruct((n, d), BF16),
            in_specs=[hbm] * 4,
            out_specs=hbm,
            scratch_shapes=[
                pltpu.VMEM((CHUNK, d), BF16),
                pltpu.VMEM((CHUNK, ff), BF16),
                pltpu.VMEM((2, d, GU), BF16),
                pltpu.VMEM((2, d, GU), BF16),
                pltpu.VMEM((2, ff, DN), BF16),
                *[pltpu.VMEM((CHUNK, GU), F32)] * 4,
                *[pltpu.VMEM((CHUNK, DN), F32)] * 2,
                pltpu.VMEM((TILES // 2 + 1, CHUNK, DN), BF16),
                pltpu.VMEM((FIRST + 1, CHUNK, DN), BF16),
                pltpu.VMEM((4, CHUNK, DN), BF16),
                pltpu.VMEM((STAGED + 1, CHUNK, DN), BF16),
                pltpu.VMEM((CHUNK, 2 * DN), BF16),
                dma, dma((2,)), dma((2,)), dma((2,)),
                dma((STAGED,)),
                dma((chunks, TILES // 2)),
                dma((chunks, FIRST + 4)),
                dma((10,)),
                dma((chunks, 9)),
                pltpu.SemaphoreType.REGULAR((3,)),
            ],
            compiler_params=pltpu.CompilerParams(
                collective_id=0, has_side_effects=True, vmem_limit_bytes=67043328),
            cost_estimate=pl.CostEstimate(flops=6 * n * d * ff, bytes_accessed=chunks * 6 * d * ff, transcendentals=n * ff),
        )(x, w_gate, w_up, w_down)

    return jax.shard_map(
        step,
        mesh=mesh,
        in_specs=(P("dp", None), P(None, "tp"), P(None, "tp"), P("tp", None)),
        out_specs=P("dp", None),
        check_vma=False,
    )
```

```python
import functools

import jax
import jax.numpy as jnp
from jax import lax
from jax.experimental import pallas as pl
from jax.experimental.pallas import tpu as pltpu
from jax.sharding import PartitionSpec as P

MESH = pl.DeviceIdType.MESH
BF16, F32 = jnp.bfloat16, jnp.float32

GU = 256
DN = 512
SHARES = (18, 18, 17, 11)
SLOTS = 6

OTHER, OWN = 0, 1
ORDER = (
    (OTHER, 2, 0), (OTHER, 2, 1), (OTHER, 3, 0), (OWN, 2, 0), (OWN, 2, 1), (OTHER, 3, 1), (OTHER, 1, 0), (OTHER, 1, 1),
    (OWN, 3, 1), (OWN, 1, 0), (OTHER, 0, 0), (OTHER, 0, 1), (OWN, 3, 0), (OWN, 1, 1), (OWN, 0, 0), (OWN, 0, 1),
)
TILES = len(ORDER)
STAGED = TILES - 2
STAGE = (0, 1, 0, 2, 3, 1, 0, 1, 4, 5, 0, 1, 6, 7)
REUSED = tuple(int(slot in STAGE[:t]) for t, slot in enumerate(STAGE))
STAGES = max(STAGE) + 1
RING = {3: (-1, 0), 4: (1, 1), 8: (-1, 3), 9: (1, 4), 12: (-1, 2), 13: (1, 5)}
FIRST = 2


def pick(t, values):
    out = jnp.int32(values[0])
    for k, v in enumerate(values[1:], 1):
        if v != values[0]:
            out = jnp.where(t == k, jnp.int32(v), out)
    return out


def kernel(chips, sizes, x_ref, wg_ref, wu_ref, wd_ref, y_ref, x_v, hid, w_v, kept, other, hop1, hop2, stage, fin,
           x_sem, w_sem, send_sem, other_sem, ring_sem, gsend_sem, gather_sem, credit):
    dp, tp = lax.axis_index("dp"), lax.axis_index("tp")
    chip, core = tp // 2, tp % 2
    nxt, prv = (chip + 1) % chips, (chip + chips - 1) % chips
    far = (chip + 2) % chips
    dev_next, dev_prev, dev_other = (dp, nxt * 2 + core), (dp, prv * 2 + core), (dp, chip * 2 + 1 - core)
    n_gu = wg_ref.shape[1] // GU
    ff = wd_ref.shape[0]
    chunks = len(sizes)
    starts = [sum(sizes[:k]) for k in range(chunks)]
    last = chunks - 1

    barrier = pltpu.get_barrier_semaphore()
    for dev in (dev_next, dev_prev, dev_other):
        pl.semaphore_signal(barrier, inc=1, device_id=dev, device_id_type=MESH)
    pl.semaphore_wait(barrier, 3)

    def x_copy(c):
        return pltpu.make_async_copy(x_ref.at[pl.ds(starts[c], sizes[c]), :], x_v.at[pl.ds(0, sizes[c]), :], x_sem)

    def w_copy(src, j, slot):
        cols = pl.ds(pl.multiple_of(j * GU, GU), GU)
        return pltpu.make_async_copy(src.at[:, cols], w_v.at[slot], w_sem.at[slot])

    def block(half, owner, piece):
        return (half * chips + owner) * 2 + piece

    def wd_load(t):
        slot = (2 * n_gu + t) % SLOTS
        half = jnp.where(pick(t, [o[0] for o in ORDER]) == OWN, core, 1 - core)
        owner = (chip + pick(t, [o[1] for o in ORDER])) % chips
        tile = block(half, owner, pick(t, [o[2] for o in ORDER]))
        for k in range(2):
            cols = pl.ds(pl.multiple_of(tile * DN + k * GU, GU), GU)
            pltpu.make_async_copy(wd_ref.at[:, cols], w_v.at[slot, pl.ds(k * ff, ff), :], w_sem.at[slot]).start()

    def w_wait(slot):
        w_copy(wg_ref, 0, slot).wait()

    def gu_load(j):
        for k, src in enumerate((wg_ref, wu_ref)):
            w_copy(src, j, (2 * j + k) % SLOTS).start()

    def remote(src, dst, send, recv, dev):
        return pltpu.make_async_remote_copy(src_ref=src, dst_ref=dst, send_sem=send, recv_sem=recv, device_id=dev,
                                            device_id_type=MESH)

    def top(ref, k, c):
        return ref.at[k, pl.ds(0, sizes[c]), :]

    def other_copy(c, t, slot):
        at = pick(t, STAGE)
        return remote(top(stage, at, c), top(other, slot, c), send_sem.at[at], other_sem.at[c, slot], dev_other)

    def ring_copy(c, t):
        direction, slot = RING[t]
        dst = top(hop1, slot, c) if slot < FIRST else top(hop2, slot - FIRST, c)
        return remote(top(stage, STAGE[t], c), dst, send_sem.at[STAGE[t]], ring_sem.at[c, slot],
                      dev_next if direction > 0 else dev_prev)

    def stage_sent(c, slot):
        remote(top(stage, slot, c), top(other, 0, c), send_sem.at[slot], other_sem.at[c, 0], dev_other).wait_send()

    def out(c, owner, half=None, piece=None):
        half = core if half is None else half
        r = pl.ds(starts[c], sizes[c])
        if piece is None:
            return y_ref.at[r, pl.ds(pl.multiple_of(block(half, owner, 0) * DN, 2 * DN), 2 * DN)]
        return y_ref.at[r, pl.ds(pl.multiple_of(block(half, owner, piece) * DN, DN), DN)]

    def gather(c, k):
        def put(src, dst, dev):
            return remote(src, dst, gsend_sem.at[k], gather_sem.at[c, k], dev)

        def mine(piece):
            return fin.at[pl.ds(0, sizes[c]), pl.ds(piece * DN, DN)], out(c, chip, piece=piece)

        if k < 4:
            piece, dev = ((0, dev_next), (1, dev_prev), (1, dev_next), (0, dev_prev))[k]
            return put(*mine(piece), dev)
        if k == 4:
            return put(fin.at[pl.ds(0, sizes[c]), :], out(c, chip), dev_other)
        if k < 7:
            owner, piece, dev = ((prv, 0, dev_next), (nxt, 1, dev_prev))[k - 5]
        else:
            owner, piece, dev = ((prv, None, dev_other), (nxt, None, dev_other), (far, 0, dev_other),
                                 (far, 1, dev_other))[k - 7]
        ref = out(c, owner, piece=piece)
        return put(ref, ref, dev)

    def gather_wait(c, k, dst):
        remote(dst, dst, gsend_sem.at[k], gather_sem.at[c, k], dev_other).wait_recv()

    def local_copy(c):
        return pltpu.make_async_copy(fin.at[pl.ds(0, sizes[c]), :], out(c, chip), gsend_sem.at[11])

    def sent(c):
        local_copy(c).wait()
        for k in range(11):
            gather(c, k).wait_send()

    def finish(c):
        for slot in range(2):
            other_wait(c, slot)
        for k in range(4):
            ring_wait(c, FIRST + k)
        size, step = sizes[c], 32

        def strip(i, _):
            r = pl.ds(pl.multiple_of(i * step, step), step)
            for piece in range(2):
                total = kept[piece, r, :] + other[piece, r, :].astype(F32)
                total += hop2[piece, r, :].astype(F32)
                total += hop2[2 + piece, r, :].astype(F32)
                fin[r, piece * DN:(piece + 1) * DN] = total.astype(BF16)
            return 0

        lax.fori_loop(0, size // step, strip, 0)
        for k in range(5):
            gather(c, k).start()
        local_copy(c).start()
        for slot in range(STAGES):
            stage_sent(c, slot)
        if c < last:
            for k, dev in enumerate((dev_prev, dev_next, dev_other)):
                pl.semaphore_signal(credit.at[k], inc=1, device_id=dev, device_id_type=MESH)

    def other_wait(c, slot):
        remote(top(stage, 0, c), top(other, slot, c), send_sem.at[0], other_sem.at[c, slot], dev_other).wait_recv()

    def ring_wait(c, slot):
        dst = top(hop1, slot, c) if slot < FIRST else top(hop2, slot - FIRST, c)
        remote(top(stage, 0, c), dst, send_sem.at[0], ring_sem.at[c, slot], dev_next).wait_recv()

    def forward1(c):
        gather_wait(c, 0, out(c, prv, piece=0))
        gather(c, 5).start()
        gather_wait(c, 1, out(c, nxt, piece=1))
        gather(c, 6).start()
        gather_wait(c, 2, out(c, prv, piece=1))
        gather(c, 7).start()
        gather_wait(c, 3, out(c, nxt, piece=0))
        gather(c, 8).start()

    def forward2(c):
        gather_wait(c, 5, out(c, far, piece=0))
        gather(c, 9).start()
        gather_wait(c, 6, out(c, far, piece=1))
        gather(c, 10).start()

    x_copy(0).start()
    for j in range(SLOTS // 2):
        gu_load(j)
    other[TILES // 2] = jnp.zeros(other.shape[1:], BF16)
    hop1[FIRST] = jnp.zeros(hop1.shape[1:], BF16)

    def one_chunk(c):
        size = sizes[c]
        span = (3, 9, 13) if size * 4 >= sizes[c - 1] * 3 else (4, 13, 15)
        x_copy(c).wait()

        def gu_step(j, _):
            @pl.when(j > 0)
            def _():
                @pl.when(j + 2 < n_gu)
                def _():
                    gu_load(j + 2)

                @pl.when(j + 2 >= n_gu)
                def _():
                    wd_load(2 * (j + 2 - n_gu))
                    wd_load(2 * (j + 2 - n_gu) + 1)

            if c:
                @pl.when(j == 0)
                def _():
                    w_copy(wu_ref, 2, 5).start()

                for at, act in zip(span, (finish, forward1, forward2)):
                    @pl.when(j == at)
                    def _(act=act):
                        act(c - 1)

            a, b = (2 * j) % SLOTS, (2 * j + 1) % SLOTS
            w_wait(a)
            w_wait(b)
            rows = x_v[:size, :]
            gate = jnp.dot(rows, w_v[a], preferred_element_type=F32)
            up = jnp.dot(rows, w_v[b], preferred_element_type=F32)
            hid[:size, pl.ds(pl.multiple_of(j * GU, GU), GU)] = (gate * jax.nn.sigmoid(gate) * up).astype(BF16)
            return 0

        lax.fori_loop(0, n_gu, gu_step, 0)

        if c:
            sent(c - 1)
            for k in range(3):
                pl.semaphore_wait(credit.at[k], 1)
        if c < last:
            x_copy(c + 1).start()

        def dn_dots(t):
            slot = (2 * n_gu + t) % SLOTS

            @pl.when(t == 0)
            def _():
                wd_load(t + 4)
                wd_load(t + 5)

            @pl.when((t > 0) & (t + 5 < TILES))
            def _():
                wd_load(t + 5)

            if c < last:
                for m in range(SLOTS - 1):
                    @pl.when(t + 5 == TILES + m)
                    def _(m=m):
                        w_copy((wg_ref, wu_ref)[m % 2], m // 2, m).start()

            w_wait(slot)
            return [jnp.dot(hid[:size, :], w_v[slot, k * ff:(k + 1) * ff, :], preferred_element_type=F32)
                    for k in range(2)]

        def dn_step(t, _):
            own = pick(t, [o[0] for o in ORDER[:STAGED]]) == OWN
            arrived = pick(t, [o[1] * 2 + o[2] for o in ORDER[:STAGED]])
            to = pick(t, STAGE)

            @pl.when(pick(t, REUSED) == 1)
            def _():
                stage_sent(c, to)

            @pl.when(own)
            def _():
                other_wait(c, arrived)

            for k, at in ((0, 12), (1, 13)):
                @pl.when(t == at)
                def _(k=k):
                    ring_wait(c, k)

            from_other = jnp.where(own, arrived, TILES // 2)
            from_ring = jnp.where(t == 12, 0, jnp.where(t == 13, 1, FIRST))
            for k, part in enumerate(dn_dots(t)):
                cols = slice(k * GU, (k + 1) * GU)
                total = part + other[from_other, :size, cols].astype(F32) + hop1[from_ring, :size, cols].astype(F32)
                stage[to, :size, cols] = total.astype(BF16)

            @pl.when(jnp.logical_not(own))
            def _():
                other_copy(c, t, arrived).start()

            for at in RING:
                @pl.when(t == at)
                def _(at=at):
                    ring_copy(c, at).start()

            return 0

        def dn_own(t, _):
            for k, part in enumerate(dn_dots(t)):
                kept[t - STAGED, :size, k * GU:(k + 1) * GU] = part
            return 0

        lax.fori_loop(0, STAGED, dn_step, 0)
        lax.fori_loop(STAGED, TILES, dn_own, 0)

    for c in range(chunks):
        one_chunk(c)
    finish(last)
    forward1(last)
    forward2(last)
    sent(last)
    half = 1 - core
    for c in range(chunks):
        for k, dst in ((4, out(c, chip, half)), (7, out(c, prv, half)), (8, out(c, nxt, half)),
                       (9, out(c, far, half, 0)), (10, out(c, far, half, 1))):
            gather_wait(c, k, dst)


def solution(mesh):
    chips = mesh.shape["tp"] // 2

    def step(x, w_gate, w_up, w_down):
        n, d = x.shape
        ff = w_gate.shape[1]
        sizes = tuple(share * n // sum(SHARES) for share in SHARES)
        chunks, size = len(sizes), max(sizes)
        dma = pltpu.SemaphoreType.DMA
        hbm = pl.BlockSpec(memory_space=pl.ANY)
        return pl.pallas_call(
            functools.partial(kernel, chips, sizes),
            out_shape=jax.ShapeDtypeStruct((n, d), BF16),
            in_specs=[hbm] * 4,
            out_specs=hbm,
            scratch_shapes=[
                pltpu.VMEM((size, d), BF16),
                pltpu.VMEM((size, ff), BF16),
                pltpu.VMEM((SLOTS, d, GU), BF16),
                pltpu.VMEM((2, size, DN), F32),
                pltpu.VMEM((TILES // 2 + 1, size, DN), BF16),
                pltpu.VMEM((FIRST + 1, size, DN), BF16),
                pltpu.VMEM((4, size, DN), BF16),
                pltpu.VMEM((STAGES, size, DN), BF16),
                pltpu.VMEM((size, 2 * DN), BF16),
                dma, dma((SLOTS,)),
                dma((STAGES,)),
                dma((chunks, TILES // 2)),
                dma((chunks, FIRST + 4)),
                dma((12,)),
                dma((chunks, 11)),
                pltpu.SemaphoreType.REGULAR((3,)),
            ],
            compiler_params=pltpu.CompilerParams(
                collective_id=0, has_side_effects=True, vmem_limit_bytes=67043328),
            cost_estimate=pl.CostEstimate(flops=6 * n * d * ff, bytes_accessed=chunks * 6 * d * ff, transcendentals=n * ff),
        )(x, w_gate, w_up, w_down)

    return jax.shard_map(
        step,
        mesh=mesh,
        in_specs=(P("dp", None), P(None, "tp"), P(None, "tp"), P("tp", None)),
        out_specs=P("dp", None),
        check_vma=False,
    )
```
